32 devices in a mesh: section: 4 (over y, core), dp: 8 (over z, x).
Axes of the slice: x: 2, y: 2, z: 4, core: 2. Of those that a mesh axis runs over, the one named last changes fastest.
Arguments:
- acts: bfloat16 [4, 4096, 3584], P('section', 'dp'), may hold values from -400 to 400
- cotangent: bfloat16 [4096, 3584], P('dp'), may hold values from -6 to 6
- frozen: bfloat16 [4, 3584, 3584], P('section', 'dp'), may hold values from -0.09375 to 0.09375
- down_adapter: bfloat16 [4, 16, 3584], P('section'), may hold values from -0.25 to 0.25
- up_adapter: bfloat16 [4, 16, 3584], P('section'), may hold values from -0.25 to 0.25
- example_ids: int32 [8, 4], P('dp'), may hold values from 0 to 3, each once within a row
- lengths: int32 [8, 4], P('dp'), may hold values from 32 to 128
Outputs:
- grad_down: float32 [4, 16, 3584], P('section', None, 'dp')
- grad_up: float32 [4, 16, 3584], P('section', None, 'dp')
- example_norms: float32 [8, 4], P('dp')
The draws below stay inside these ranges and needn't reach their ends.
Inputs may be any that keep to these rules, and one draw needn't show every extreme that they name: `example_ids`: each row is an ordering of the 4 examples of one replica.
All inputs are finite; a program needn't handle non-finite values.
Results may differ from the reference program's by a relative error of at most 0.009.
Values may be sent and summed in bfloat16 or wider, within the bound.
No kernel may reach another device: no remote copies, remote signals or barrier semaphores. Data moves between devices by JAX's collectives and lax.ppermute only.
A program may use at most 128 MiB of HBM per device.

```python
import math
import jax
import jax.numpy as jnp
from jax import lax

DW = 3584
RANK = 16
MICRO = 4
SEQ = 128
SECTIONS = 4
REPLICAS = 8
EXAMPLES = 32
TOKENS = 4096


def draw_acts(key, part):
    keys = jax.random.split(jax.random.fold_in(key, 17), 4)
    section_pos = jnp.arange(SECTIONS, dtype=jnp.float32) / max(SECTIONS - 1, 1)
    base = jax.random.truncated_normal(keys[0], -4.0, 4.0, (SECTIONS, TOKENS, DW), jnp.float32)
    section_scale = 3.0 ** section_pos
    row_scale = jnp.exp(jax.random.uniform(keys[2], (SECTIONS, TOKENS, 1), jnp.float32, -1.15, 1.15))
    col_scale = jnp.exp(jax.random.uniform(keys[3], (SECTIONS, 1, DW), jnp.float32, -1.15, 1.15))
    return (base * row_scale * col_scale * section_scale[:, None, None]).astype(jnp.bfloat16)


def touch_ends(values, stream_key, smallest, high):
    longest = values.shape.index(max(values.shape))
    spots = []
    for shift in (0, 1):
        where = [jax.random.randint(jax.random.fold_in(stream_key, axis), (), 0, length) for axis, length in enumerate(values.shape)]
        where[longest] = (where[longest] + shift) % values.shape[longest]
        spots.append(tuple(where))
    return values.at[spots[0]].set(smallest).at[spots[1]].set(high)


def block_scale(own_key, dims, pieces, least, top_value):
    def one(dim, blocks):
        heights = jax.random.uniform(jax.random.fold_in(jax.random.fold_in(own_key, 6), dim), (blocks,), jnp.float32, least / len(pieces), top_value / len(pieces))
        return jnp.repeat(jnp.exp(heights), dims[dim] // blocks).reshape((-1,) + (1,) * (len(dims) - dim - 1))

    factor_of = one(*pieces[0])
    for cut in pieces[1:]:
        factor_of = factor_of * one(*cut)
    return factor_of


def scatter_about(own_key, dims, deviation, most, shards=(), kind=jnp.bfloat16):
    array = deviation * jax.random.normal(own_key, dims, jnp.float32)
    if shards:
        array = array * block_scale(own_key, dims, shards, -0.22, 0.18)
    return jnp.clip(array, -most, most).astype(kind)


def setup_inputs(seed: int = 0) -> dict:
    seeds = jax.random.split(jax.random.key(seed), 8)
    acts = draw_acts(jax.random.fold_in(seeds[7], 71), 0)
    cotangent = scatter_about(seeds[1], (TOKENS, DW), 1.0, 6.0, ((0, 8),))
    frozen = scatter_about(seeds[2], (SECTIONS, DW, DW), (DW * 5 // 4) ** -0.5, 0.09375, ((0, 4), (1, 8)))
    down_adapter = scatter_about(seeds[3], (SECTIONS, RANK, DW), ((5 * RANK * DW) ** 0.5) ** -0.5, 0.25, ((0, 4),))
    up_adapter = scatter_about(seeds[4], (SECTIONS, RANK, DW), ((5 * RANK * DW) ** 0.5) ** -0.5, 0.25, ((0, 4),))
    example_ids = jax.vmap(lambda own: jax.random.permutation(own, MICRO))(jax.random.split(seeds[5], REPLICAS)).reshape((REPLICAS, MICRO)).astype(jnp.int32)
    lengths = touch_ends(jax.random.randint(seeds[6], (REPLICAS, MICRO), SEQ // 4, SEQ + 1), jax.random.fold_in(seeds[6], 1), SEQ // 4, SEQ).astype(jnp.int32)
    return {"acts": acts, "cotangent": cotangent, "frozen": frozen, "down_adapter": down_adapter, "up_adapter": up_adapter, "example_ids": example_ids, "lengths": lengths}


def reference(acts, cotangent, frozen, down_adapter, up_adapter, example_ids, lengths):
    choose = (example_ids[:, :, None] == jnp.arange(MICRO, dtype=jnp.int32)[None, None, :]).astype(jnp.int32)
    slot_length = lax.optimization_barrier(jnp.sum(choose * lengths[:, None, :], axis=2))
    live = (jnp.arange(SEQ, dtype=jnp.int32)[None, None, :] < slot_length[:, :, None]).astype(jnp.bfloat16)
    out_grad = cotangent * live.reshape(TOKENS, 1)
    down_terms = []
    up_terms = []
    square_sum = jnp.zeros((EXAMPLES,), jnp.float32)
    for section in range(SECTIONS - 1, -1, -1):
        inputs = acts[section]
        up_grad = jnp.dot(out_grad, up_adapter[section].T, preferred_element_type=jnp.float32).astype(jnp.bfloat16)
        down_act = jnp.dot(inputs, down_adapter[section].T, preferred_element_type=jnp.float32).astype(jnp.bfloat16)
        down_term = jnp.einsum('esr,esd->erd', up_grad.reshape(EXAMPLES, SEQ, RANK).astype(jnp.float32), inputs.reshape(EXAMPLES, SEQ, DW).astype(jnp.float32))
        up_term = jnp.einsum('esr,esd->erd', down_act.reshape(EXAMPLES, SEQ, RANK).astype(jnp.float32), out_grad.reshape(EXAMPLES, SEQ, DW).astype(jnp.float32))
        square_sum = square_sum + lax.optimization_barrier(jnp.sum(down_term * down_term, axis=(1, 2))) + lax.optimization_barrier(jnp.sum(up_term * up_term, axis=(1, 2)))
        down_terms.append(down_term)
        up_terms.append(up_term)
        in_grad = jnp.dot(out_grad, frozen[section].T, preferred_element_type=jnp.float32)
        in_grad = in_grad + jnp.dot(up_grad, down_adapter[section], preferred_element_type=jnp.float32)
        out_grad = in_grad.astype(jnp.bfloat16)
    norm = jnp.sqrt(square_sum)
    factor = math.sqrt(2.0 * RANK * DW) / ((norm + 0.01) * math.sqrt(EXAMPLES))
    down_terms = down_terms[::-1]
    up_terms = up_terms[::-1]
    grad_down = jnp.stack([lax.optimization_barrier(jnp.sum(factor[:, None, None] * term, axis=0)) for term in down_terms])
    grad_up = jnp.stack([lax.optimization_barrier(jnp.sum(factor[:, None, None] * term, axis=0)) for term in up_terms])
    slot_norm = norm.reshape(REPLICAS, MICRO)
    example_norms = lax.optimization_barrier(jnp.sum(choose.astype(jnp.float32) * slot_norm[:, :, None], axis=1))
    return (grad_down, grad_up, example_norms)
```

```python
import math

import jax
import jax.numpy as jnp
from jax import lax
from jax.experimental import pallas as pl
from jax.experimental.pallas import tpu as pltpu
from jax.sharding import Mesh, PartitionSpec as P

LANES = 128
BF16 = jnp.bfloat16
F32 = jnp.float32
VMEM = pl.BlockSpec(memory_space=pltpu.VMEM)
SMEM = pl.BlockSpec(memory_space=pltpu.SMEM)


def mm(left, right, dims):
    return lax.dot_general(left, right, (dims, ((), ())), preferred_element_type=F32)


def nt(left, right):
    return mm(left, right, ((1,), (1,)))


def nn(left, right):
    return mm(left, right, ((1,), (0,)))


def local_call(body, where, arrays, shapes, scratch=(), specs=None):
    specs = [VMEM] * len(arrays) if specs is None else specs
    return pl.pallas_call(
        body,
        out_shape=shapes,
        grid=(1,),
        in_specs=[SMEM] + specs,
        out_specs=[VMEM] * len(shapes),
        scratch_shapes=list(scratch),
        compiler_params=pltpu.CompilerParams(vmem_limit_bytes=56 * 1024 * 1024),
    )(where, *arrays)


def shape_of(dims, dtype=BF16):
    return jax.ShapeDtypeStruct(dims, dtype)


def xor_permute(value, axes, count, step):
    return lax.ppermute(value, axes, [(i, i ^ step) for i in range(count)])


class Plan:
    def __init__(self, sizes, features, rank, slots, positions, block):
        self.ny, self.nc, self.nz, self.nx = sizes
        self.sections, self.replicas = self.ny * self.nc, self.nz * self.nx
        self.quarters = self.ny * self.nx
        self.features, self.rank, self.slots, self.positions = features, rank, slots, positions
        self.block = block
        self.part = features // self.nz
        self.width = -(-self.part // (self.quarters * LANES)) * LANES
        self.wide = self.nz * self.width
        self.half = slots // self.nc
        self.group = self.half * rank
        self.height = self.group * self.replicas

    def window(self, replica):
        low = replica * self.block // LANES * LANES
        return low, min(-(-self.block // LANES) * LANES, self.features - low)

    def lane(self, quarter, step):
        low = quarter * self.width + step * LANES
        return jnp.minimum(low, self.part - LANES), low < self.part


def cut_weight(plan, where, weight_ref, *outs):
    quarter, iz = where[0], where[1]
    for k, out in enumerate(outs):
        for m in range(plan.nz):
            for h in range(plan.width // LANES):
                low, _ = plan.lane(quarter ^ k, h)
                start = pl.multiple_of((iz ^ m) * plan.part + low, LANES)
                lanes = slice(m * plan.width + h * LANES, m * plan.width + (h + 1) * LANES)
                out[:, lanes] = weight_ref[:, pl.ds(start, LANES)]


def sort_adapters(plan, where, *refs):
    quarter, iz, section = where[0], where[1], where[2]
    ins, (up_quarter, up_part, down_part) = refs[: plan.sections], refs[plan.sections :]
    for j, known in enumerate(ins):
        s = section ^ j
        for m in range(plan.nz):
            for h in range(plan.width // LANES):
                low, _ = plan.lane(quarter, h)
                start = pl.multiple_of((iz ^ m) * plan.part + low, LANES)
                lanes = slice(m * plan.width + h * LANES, m * plan.width + (h + 1) * LANES)
                up_quarter[s, :, lanes] = known[:, pl.ds(start, LANES)]
        start = pl.multiple_of(iz * plan.part, LANES)
        up_part[s] = known[:, pl.ds(start, plan.part)]
        down_part[s] = known[:, plan.features :]


def collect(plan, where, *refs):
    for k in range(plan.quarters):
        refs[plan.quarters][where[0] ^ k] = refs[k][...]


def first_rows(plan, where, *refs):
    iz, section, iy, ic, ix, replica = where[1], where[2], where[3], where[4], where[5], where[6]
    tokens = plan.slots * plan.positions
    known_acts = refs[: plan.sections]
    grad, weight, up_rows, own_down, low_out, high_out, act, rows, seeds = refs[plan.sections :]
    for j, known in enumerate(known_acts):
        act[section ^ j] = known[...]
    for i in range(plan.half):
        start = pl.multiple_of((ic * plan.half + i) * plan.positions, plan.positions)
        left = jnp.concatenate([act[s, :, pl.ds(start, plan.positions)] for s in range(plan.sections - 1)], axis=0)
        for m in range(plan.nz):
            lanes = pl.multiple_of((iz ^ m) * plan.part, LANES)
            right = grad[pl.ds(start, plan.positions), pl.ds(lanes, plan.part)]
            made = nn(left, right).astype(BF16)
            for s in range(plan.sections - 1):
                low = s * plan.group + i * plan.rank
                rows[m, low : low + plan.rank, :] = made[s * plan.rank : (s + 1) * plan.rank]
    start_rows = act[0, :, tokens : tokens + plan.block]
    seed = nn(start_rows, weight[...]) + nn(nt(start_rows, own_down[...]).astype(BF16), up_rows[...])
    seeds[...] = seed.astype(BF16)
    for d in range(plan.replicas):
        low, window = plan.window(d)
        low_out[d, plan.group :, :window] = seeds[:, low : low + window]
    for kx in range(plan.nx):
        quarter = iy * plan.nx + (ix ^ kx)
        for m in range(plan.nz):
            for h in range(plan.width // LANES):
                low, there = plan.lane(quarter, h)
                tile = rows[m, :, pl.ds(pl.multiple_of(low, LANES), LANES)]
                tile = jnp.where(there, tile, jnp.zeros_like(tile))
                for kz in range(plan.nz):
                    at = (kz ^ m) * plan.width + h * LANES
                    there_index = replica ^ (kz * plan.nx + kx)
                    low_out[there_index, : plan.group, at : at + LANES] = tile[: plan.group]
                    high_out[there_index, :, at : at + LANES] = tile[plan.group :]


def stage_rows(plan, t, count, where, *refs):
    quarter, ic = where[0], where[4]
    pieces = refs[:count]
    mine, twin, up_quarter, down_part = refs[count : count + 4]
    outs = refs[count + 4 : count + 4 + plan.quarters]
    flat, made = refs[count + 4 + plan.quarters :]
    if count == 1:
        flat = pieces[0]
    else:
        for j, piece in enumerate(pieces):
            flat[:, j * plan.width : (j + 1) * plan.width] = piece[...]
    tall = plan.height

    def compute(held):
        def tile(index, carry):
            at = pl.ds(pl.multiple_of(index * tall, tall), tall)
            rows = flat[at, :]
            bend = nt(rows, up_quarter[t]).astype(BF16)
            matrix = held[...].reshape(plan.part, plan.wide)
            for q in range(plan.quarters):
                low, high = min(q * plan.width, plan.part), min((q + 1) * plan.width, plan.part)
                if high > low:
                    value = nt(rows, matrix[low:high]) + nn(bend, down_part[t, :, low:high])
                    made[quarter ^ q, at, : high - low] = value.astype(BF16)
                if high - low < plan.width:
                    made[quarter ^ q, at, high - low :] = jnp.zeros((tall, plan.width - (high - low)), BF16)
            return carry

        lax.fori_loop(0, flat.shape[0] // tall, tile, 0)

    @pl.when(ic == t % plan.nc)
    def _():
        compute(mine)

    @pl.when(ic != t % plan.nc)
    def _():
        compute(twin)

    for k, out in enumerate(outs):
        out[...] = made[k]


def carry_rows(plan, t, count, split, where, *refs):
    quarter, ic = where[0], where[4]
    pieces = refs[:count]
    mine, twin, up_quarter, up_part, down_part = refs[count : count + 5]
    outs = refs[count + 5 : -1]
    stacked = refs[-1]
    old = (t - 1) * plan.rank
    if count == 1:
        stacked[:old, : plan.part] = pieces[0][...]
    else:
        for k, piece in enumerate(pieces):
            start = pl.multiple_of((quarter ^ k) * plan.width, LANES)
            stacked[:old, pl.ds(start, plan.width)] = piece[...]
    stacked[old:, : plan.part] = up_part[t - 1]

    def compute(held):
        rows = stacked[:, : plan.part]
        bend = nt(rows, down_part[t]).astype(BF16)
        value = nn(rows, held[...].reshape(plan.part, plan.wide)) + nn(bend, up_quarter[t])
        value = value.astype(BF16)
        if split:
            for m, out in enumerate(outs):
                out[...] = value[:, m * plan.width : (m + 1) * plan.width]
        else:
            outs[0][...] = value

    @pl.when(ic == t % plan.nc)
    def _():
        compute(mine)

    @pl.when(ic != t % plan.nc)
    def _():
        compute(twin)


def own_terms(plan, where, *refs):
    quarter, iz, section = where[0], where[1], where[2]
    pieces = refs[: plan.quarters]
    up_rows, grad, inputs, live, act = refs[plan.quarters : plan.quarters + 5]
    down_terms, top_terms, squares, carried = refs[plan.quarters + 5 :]
    last = section == plan.sections - 1
    for k, piece in enumerate(pieces):
        for m in range(plan.nz):
            for h in range(plan.width // LANES):
                low, there = plan.lane(quarter ^ k, h)
                start = pl.multiple_of((iz ^ m) * plan.part + low, LANES)

                @pl.when(there)
                def _():
                    at = m * plan.width + h * LANES
                    carried[:, pl.ds(start, LANES)] = piece[:, at : at + LANES]

    @pl.when(last)
    def _():
        carried[...] = up_rows[...]

    up_grad = (nt(carried[...], grad[...]).astype(BF16).astype(F32) * live[...]).astype(BF16)
    for m in range(plan.slots):
        where_rows = slice(m * plan.positions, (m + 1) * plan.positions)
        down = nn(up_grad[:, where_rows], inputs[where_rows, :])
        top = nn(act[:, where_rows], grad[where_rows, :])
        down_terms[m] = down
        top_terms[m] = top
        total = jnp.sum(down * down) + jnp.where(last, jnp.sum(top * top), 0.0)
        squares[m : m + 1, :] = jnp.full((1, LANES), total, F32)


def on_device(acts, cotangent, frozen, down_adapter, up_adapter, example_ids, lengths):
    sizes = [lax.axis_size(name) for name in ("y", "c", "z", "x")]
    ny, nc, nz, nx = sizes
    iy, ic, iz, ix = (lax.axis_index(name) for name in ("y", "c", "z", "x"))
    inputs, weight = acts[0], frozen[0]
    down_rows, up_rows = down_adapter[0], up_adapter[0]
    slots = example_ids.shape[1]
    tokens, features = inputs.shape
    positions, rank, block = tokens // slots, down_rows.shape[0], weight.shape[0]
    plan = Plan(sizes, features, rank, slots, positions, block)
    sections, replicas, quarters = plan.sections, plan.replicas, plan.quarters
    part, width, wide, half = plan.part, plan.width, plan.wide, plan.half
    section = iy * nc + ic
    quarter = iy * nx + ix
    replica = iz * nx + ix
    where = jnp.stack([quarter, iz, section, iy, ic, ix, replica]).astype(jnp.int32)
    last = section == sections - 1

    def run(body, arrays, shapes, scratch=(), specs=None, extra=(), after=()):
        def kernel(at, *refs):
            body(plan, *extra, at, *refs[len(after) :])

        specs = [VMEM] * len(arrays) if specs is None else specs
        specs = [pl.BlockSpec(memory_space=pl.ANY)] * len(after) + specs
        arrays = list(after) + list(arrays)
        return local_call(kernel, where, arrays, shapes, scratch, specs)

    choose = (example_ids[0][:, None] == jnp.arange(slots, dtype=jnp.int32)[None, :]).astype(jnp.int32)
    slot_length = jnp.sum(choose * lengths[0][None, :], axis=1)
    live = jnp.arange(positions, dtype=jnp.int32)[None, :] < slot_length[:, None]
    live = live.astype(F32).reshape(1, tokens)
    clip_scale = math.sqrt(2.0 * rank * features) / math.sqrt(replicas * slots)

    down_act = (nt(down_rows, inputs).astype(BF16).astype(F32) * live).astype(BF16)
    own_up = lax.dynamic_slice_in_dim(up_rows, replica * block, block, 1)
    own_down = lax.dynamic_slice_in_dim(down_rows, replica * block, block, 1)
    act_known = jnp.concatenate([down_act, own_up], axis=1)
    act_all = [act_known] + [xor_permute(act_known, ("y", "c"), sections, j) for j in range(1, sections)]

    def cut(after):
        return run(cut_weight, [weight], [shape_of((block, wide))] * quarters, after=after)

    pieces = cut(act_all[1:])

    outs = run(
        first_rows,
        act_all + [cotangent, weight, up_rows, own_down],
        [
            shape_of((replicas, plan.group + rank, wide)),
            shape_of((replicas, (sections - 2) * plan.group, wide)),
        ],
        scratch=[
            pltpu.VMEM((sections, rank, tokens + block), BF16),
            pltpu.VMEM((nz, (sections - 1) * plan.group, part), BF16),
            pltpu.VMEM((rank, features), BF16),
        ],
        after=[pieces[1]],
    )
    lead = lax.all_to_all(outs[0], ("z", "x"), split_axis=0, concat_axis=0)

    def send_weight(pieces, core, step):
        pairs = []
        for y in range(ny):
            for x in range(nx):
                if y * nc + core > 0:
                    other = (y * nx + x) ^ step
                    pairs.append(
                        (((y * nc + core) * nx) + x, ((other // nx) * nc + core) * nx + other % nx)
                    )
        return lax.ppermute(pieces[step], ("y", "c", "x"), pairs)

    start = lax.dynamic_slice_in_dim(down_rows, iz * part, part, 1)
    adapters = jnp.concatenate([up_rows, start], axis=1)
    known = [adapters] + [xor_permute(adapters, ("y", "c"), sections, j) for j in range(1, sections)]
    up_quarter, up_part, down_part = run(
        sort_adapters,
        known,
        [shape_of((sections, rank, wide)), shape_of((sections, rank, part)), shape_of((sections, rank, part))],
        after=[outs[0]],
    )

    own, twin = {}, {}

    later = cut([outs[0]])

    def share(core, pieces, after):
        held = [pieces[0]] + [send_weight(pieces, core, step) for step in range(1, quarters)]
        (own[core],) = run(collect, held, [shape_of((quarters, block, wide))], after=after)
        twin[core] = lax.ppermute(own[core], "c", [(core, c) for c in range(nc) if c != core])

    share(nc - 1, pieces, [up_quarter, later[1]])

    def weight_specs(t):
        y = t // nc
        spec = pl.BlockSpec((nx, block, wide), lambda i: (y, 0, 0))
        return [spec, spec]

    finals = {}

    def stage(t, rows, after=()):
        count, height = len(rows), rows[0].shape[0]
        made = run(
            stage_rows,
            rows + [own[t % nc], twin[t % nc], up_quarter, down_part],
            [shape_of((height, width))] * quarters,
            scratch=[
                pltpu.VMEM((height if count > 1 else 8, wide), BF16),
                pltpu.VMEM((quarters, height, width), BF16),
            ],
            specs=[VMEM] * count + weight_specs(t) + [VMEM, VMEM],
            extra=(t, count),
            after=after,
        )
        total = made[0].astype(F32)
        for step in range(1, quarters):
            total = total + xor_permute(made[step], ("y", "x"), quarters, step).astype(F32)
        return total, made[0]

    def to_parts(keep):
        mine = keep.astype(BF16)
        return [mine] + [xor_permute(mine, "z", nz, m) for m in range(1, nz)]

    marks, sent = {}, {}
    rows = [lead[:, : plan.group].reshape(replicas * plan.group, wide)]
    for t in range(sections - 1, 0, -1):
        total, marks[t] = stage(t, rows)
        if t > 1:
            rows = to_parts(total)
            sent[t] = rows[0]
        if t == sections - 1:
            for core in range(nc - 2, -1, -1):
                share(core, later, [sent[t]])
    finals[0] = total
    rows = lax.all_to_all(outs[1], ("z", "x"), split_axis=0, concat_axis=0)
    rows = [rows.reshape(-1, wide)]
    for t in range(sections - 1, 1, -1):
        total, _ = stage(t, rows, [sent[t]])
        total = total.reshape(replicas, t - 1, plan.group, width)
        finals[t - 1] = total[:, -1]
        if t > 2:
            rows = to_parts(total[:, :-1].reshape(-1, width))

    seed = jnp.sum(lead[:, plan.group :].astype(F32), axis=0).astype(BF16)
    seed = lax.dynamic_slice_in_dim(seed, replica * block % LANES, block, 1)
    seed = jnp.where(ic == 1 % nc, seed, lax.ppermute(seed, "c", [(1 % nc, c) for c in range(nc) if c != 1 % nc]))
    seeds = [seed] + [xor_permute(seed, ("y", "x"), quarters, k) for k in range(1, quarters)]
    seeds = jnp.stack(seeds)
    home = (1 // nc) * nx
    prefix = [
        jnp.concatenate(
            [lax.dynamic_index_in_dim(seeds, quarter ^ (home + x), 0, keepdims=False) for x in range(nx)], axis=1
        )
    ]
    for t in range(2, sections):
        split = t < sections - 1
        count = len(prefix)
        height = t * rank
        made = run(
            carry_rows,
            prefix + [own[t % nc], twin[t % nc], up_quarter, up_part, down_part],
            [shape_of((height, width))] * nz if split else [shape_of((height, wide))],
            scratch=[pltpu.VMEM((height, width * quarters), BF16)],
            specs=[VMEM] * count + weight_specs(t) + [VMEM] * 3,
            extra=(t, count, split),
            after=[sent[sections + 1 - t]],
        )
        if split:
            total = made[0].astype(F32)
            for m in range(1, nz):
                total = total + xor_permute(made[m], "z", nz, m).astype(F32)
            total = total.astype(BF16)
            prefix = [total] + [xor_permute(total, ("y", "x"), quarters, k) for k in range(1, quarters)]
        else:
            total = made[0].astype(F32).reshape(height, nz, width)
            for m in range(1, nz):
                other = xor_permute(made[0], "z", nz, m).astype(F32)
                total = total + jnp.concatenate(
                    [other[:, (j ^ m) * width : ((j ^ m) + 1) * width] for j in range(nz)], axis=1
                ).reshape(height, nz, width)
            total = total.astype(BF16).reshape(sections - 1, rank, wide)
            picked = []
            for k in range(quarters):
                target = (quarter ^ k) // nx * nc + ic
                picked.append(
                    lax.dynamic_index_in_dim(total, jnp.minimum(target, sections - 2), 0, keepdims=False)
                )
            prefix = [picked[0]] + [
                xor_permute(picked[k], ("y", "x"), quarters, k) for k in range(1, quarters)
            ]

    down_terms, top_terms, own_squares = run(
        own_terms,
        prefix + [up_rows, cotangent, inputs, live, down_act],
        [shape_of((slots, rank, features), F32), shape_of((slots, rank, features), F32), shape_of((slots, LANES), F32)],
        scratch=[pltpu.VMEM((rank, features), BF16)],
        after=[marks[1]],
    )

    mine = (jnp.arange(replicas) == replica).astype(F32)[:, None] * own_squares[:, 0][None, :]
    carried = {s: finals[s].reshape(replicas, half, rank, width) for s in finals}
    squares = sum(jnp.sum(value * value, axis=(2, 3)) for value in carried.values())
    squares = (jnp.arange(nc) == ic).astype(F32)[None, :, None] * squares[:, None, :]
    squares = (mine + squares.reshape(replicas, slots)).reshape(1, 1, replicas * slots)
    squares = jnp.broadcast_to(squares, (sections * replicas, 8, replicas * slots))
    squares = lax.all_to_all(squares, ("y", "c", "z", "x"), split_axis=0, concat_axis=0)
    totals = jnp.sum(squares[:, 0], axis=0).reshape(replicas, slots)
    norms = jnp.sqrt(totals)
    factors = clip_scale / (norms + 0.01)

    own_norms = lax.dynamic_index_in_dim(norms, replica, 0, keepdims=False)
    own_factors = lax.dynamic_index_in_dim(factors, replica, 0, keepdims=False)[:, None, None]
    sums = jnp.stack([jnp.sum(own_factors * down_terms, axis=0), jnp.sum(own_factors * top_terms, axis=0)])
    sums = sums.astype(BF16).reshape(2 * rank, replicas, block).transpose(1, 0, 2)
    sums = lax.all_to_all(sums, ("z", "x"), split_axis=0, concat_axis=0)
    sums = jnp.sum(sums.astype(F32), axis=0)
    grad_down, top_up = sums[:rank], sums[rank:]

    core_factors = lax.dynamic_index_in_dim(factors.reshape(replicas, nc, half), ic, 1, keepdims=False)
    scaled = [jnp.sum(core_factors[:, :, None, None] * carried[s], axis=(0, 1)) for s in range(sections - 1)]
    scaled.append(jnp.zeros_like(scaled[0]))
    scaled = jnp.stack(scaled)
    place = section * nx + ix
    found = []
    for k in range(sections * nx):
        part_rows = lax.dynamic_index_in_dim(scaled, (place ^ k) // nx, 0, keepdims=False)
        found.append(part_rows if k == 0 else xor_permute(part_rows, ("y", "c", "x"), sections * nx, k))
    found = jnp.stack(found).reshape(ny, nc, nx, rank, width)
    found = jnp.sum(found, axis=1).reshape(quarters, rank, width)
    scaled = jnp.concatenate(
        [lax.dynamic_index_in_dim(found, quarter ^ q, 0, keepdims=False) for q in range(quarters)], axis=1
    )
    low_up = lax.dynamic_slice_in_dim(scaled, ix * block, block, 1)
    grad_up = jnp.where(last, top_up, low_up)
    example_norms = jnp.sum(choose.astype(F32) * own_norms[:, None], axis=0)
    return (grad_down[None], grad_up[None], example_norms[None])


def solution(mesh):
    sections, replicas = mesh.shape["section"], mesh.shape["dp"]
    nc = 2
    ny = sections // nc
    nx = ny
    nz = replicas // nx
    fine = Mesh(mesh.devices.reshape(ny, nc, nz, nx), ("y", "c", "z", "x"))
    section, dp = ("y", "c"), ("z", "x")
    in_specs = (
        P(section, dp, None),
        P(dp, None),
        P(section, dp, None),
        P(section, None, None),
        P(section, None, None),
        P(dp, None),
        P(dp, None),
    )
    out_specs = (P(section, None, dp), P(section, None, dp), P(dp, None))

    return jax.shard_map(on_device, mesh=fine, in_specs=in_specs, out_specs=out_specs, check_vma=False)
```

```python
import math

import jax
import jax.numpy as jnp
from jax import lax
from jax.experimental import pallas as pl
from jax.experimental.pallas import tpu as pltpu
from jax.sharding import Mesh, PartitionSpec as P

LANES = 128
BF16 = jnp.bfloat16
F32 = jnp.float32
VMEM = pl.BlockSpec(memory_space=pltpu.VMEM)
SMEM = pl.BlockSpec(memory_space=pltpu.SMEM)


def mm(left, right, dims):
    return lax.dot_general(left, right, (dims, ((), ())), preferred_element_type=F32)


def nt(left, right):
    return mm(left, right, ((1,), (1,)))


def nn(left, right):
    return mm(left, right, ((1,), (0,)))


def local_call(body, where, arrays, shapes, scratch=(), specs=None):
    specs = [VMEM] * len(arrays) if specs is None else specs
    return pl.pallas_call(
        body,
        out_shape=shapes,
        grid=(1,),
        in_specs=[SMEM] + specs,
        out_specs=[VMEM] * len(shapes),
        scratch_shapes=list(scratch),
        compiler_params=pltpu.CompilerParams(vmem_limit_bytes=56 * 1024 * 1024),
    )(where, *arrays)


def shape_of(dims, dtype=BF16):
    return jax.ShapeDtypeStruct(dims, dtype)


def xor_permute(value, axes, count, step):
    return lax.ppermute(value, axes, [(i, i ^ step) for i in range(count)])


class Plan:
    def __init__(self, sizes, features, rank, slots, positions, block):
        self.ny, self.nc, self.nz, self.nx = sizes
        self.sections, self.replicas = self.ny * self.nc, self.nz * self.nx
        self.quarters = self.ny * self.nx
        self.features, self.rank, self.slots, self.positions = features, rank, slots, positions
        self.block = block
        self.part = features // self.nz
        self.width = -(-self.part // (self.quarters * LANES)) * LANES
        self.wide = self.nz * self.width
        self.half = slots // self.nc
        self.group = self.half * rank
        self.height = self.group * self.replicas

    def window(self, replica):
        low = replica * self.block // LANES * LANES
        return low, min(-(-self.block // LANES) * LANES, self.features - low)

    def lane(self, quarter, step):
        low = quarter * self.width + step * LANES
        return jnp.minimum(low, self.part - LANES), low < self.part


def cut_weight(plan, where, weight_ref, *outs):
    quarter, iz = where[0], where[1]
    for k, out in enumerate(outs):
        for m in range(plan.nz):
            for h in range(plan.width // LANES):
                low, _ = plan.lane(quarter ^ k, h)
                start = pl.multiple_of((iz ^ m) * plan.part + low, LANES)
                lanes = slice(m * plan.width + h * LANES, m * plan.width + (h + 1) * LANES)
                out[:, lanes] = weight_ref[:, pl.ds(start, LANES)]


def sort_adapters(plan, where, *refs):
    quarter, iz, section = where[0], where[1], where[2]
    ins, (up_quarter, up_part, down_part) = refs[: plan.sections], refs[plan.sections :]
    for j, known in enumerate(ins):
        s = section ^ j
        for m in range(plan.nz):
            for h in range(plan.width // LANES):
                low, _ = plan.lane(quarter, h)
                start = pl.multiple_of((iz ^ m) * plan.part + low, LANES)
                lanes = slice(m * plan.width + h * LANES, m * plan.width + (h + 1) * LANES)
                up_quarter[s, :, lanes] = known[:, pl.ds(start, LANES)]
        start = pl.multiple_of(iz * plan.part, LANES)
        up_part[s] = known[:, pl.ds(start, plan.part)]
        down_part[s] = known[:, plan.features :]


def collect(plan, stages, where, *refs):
    pieces, outs = refs[: plan.quarters], refs[plan.quarters :]
    for k, piece in enumerate(pieces):
        source = where[0] ^ k
        for y, out in zip(stages, outs):

            @pl.when(source // plan.nx == y)
            def _():
                out[source % plan.nx] = piece[...]


def first_rows(plan, where, *refs):
    iz, section, iy, ic, ix, replica = where[1], where[2], where[3], where[4], where[5], where[6]
    tokens = plan.slots * plan.positions
    known_acts = refs[: plan.sections]
    grad, weight, up_rows, own_down, low_out, high_out, act, rows, seeds = refs[plan.sections :]
    for j, known in enumerate(known_acts):
        act[section ^ j] = known[...]
    for i in range(plan.half):
        start = pl.multiple_of((ic * plan.half + i) * plan.positions, plan.positions)
        left = jnp.concatenate([act[s, :, pl.ds(start, plan.positions)] for s in range(plan.sections - 1)], axis=0)
        for m in range(plan.nz):
            lanes = pl.multiple_of((iz ^ m) * plan.part, LANES)
            right = grad[pl.ds(start, plan.positions), pl.ds(lanes, plan.part)]
            made = nn(left, right).astype(BF16)
            for s in range(plan.sections - 1):
                low = s * plan.group + i * plan.rank
                rows[m, low : low + plan.rank, :] = made[s * plan.rank : (s + 1) * plan.rank]
    start_rows = act[0, :, tokens : tokens + plan.block]
    seed = nn(start_rows, weight[...]) + nn(nt(start_rows, own_down[...]).astype(BF16), up_rows[...])
    seeds[...] = seed.astype(BF16)
    for d in range(plan.replicas):
        low, window = plan.window(d)
        low_out[d, plan.group :, :window] = seeds[:, low : low + window]
    for kx in range(plan.nx):
        quarter = iy * plan.nx + (ix ^ kx)
        for m in range(plan.nz):
            for h in range(plan.width // LANES):
                low, there = plan.lane(quarter, h)
                tile = rows[m, :, pl.ds(pl.multiple_of(low, LANES), LANES)]
                tile = jnp.where(there, tile, jnp.zeros_like(tile))
                for kz in range(plan.nz):
                    at = (kz ^ m) * plan.width + h * LANES
                    there_index = replica ^ (kz * plan.nx + kx)
                    low_out[there_index, : plan.group, at : at + LANES] = tile[: plan.group]
                    high_out[there_index, :, at : at + LANES] = tile[plan.group :]


def stage_rows(plan, t, count, where, *refs):
    quarter, ic = where[0], where[4]
    pieces = refs[:count]
    mine, twin, up_quarter, down_part = refs[count : count + 4]
    outs = refs[count + 4 : count + 4 + plan.quarters]
    flat, made = refs[count + 4 + plan.quarters :]
    if count == 1:
        flat = pieces[0]
    else:
        for j, piece in enumerate(pieces):
            flat[:, j * plan.width : (j + 1) * plan.width] = piece[...]
    tall = plan.height

    def compute(held):
        def tile(index, carry):
            at = pl.ds(pl.multiple_of(index * tall, tall), tall)
            rows = flat[at, :]
            bend = nt(rows, up_quarter[t]).astype(BF16)
            matrix = held[...].reshape(plan.part, plan.wide)
            for q in range(plan.quarters):
                low, high = min(q * plan.width, plan.part), min((q + 1) * plan.width, plan.part)
                if high > low:
                    value = nt(rows, matrix[low:high]) + nn(bend, down_part[t, :, low:high])
                    made[quarter ^ q, at, : high - low] = value.astype(BF16)
                if high - low < plan.width:
                    made[quarter ^ q, at, high - low :] = jnp.zeros((tall, plan.width - (high - low)), BF16)
            return carry

        lax.fori_loop(0, flat.shape[0] // tall, tile, 0)

    @pl.when(ic == t % plan.nc)
    def _():
        compute(mine)

    @pl.when(ic != t % plan.nc)
    def _():
        compute(twin)

    for k, out in enumerate(outs):
        out[...] = made[k]


def carry_rows(plan, t, count, split, where, *refs):
    quarter, ic = where[0], where[4]
    pieces = refs[:count]
    mine, twin, up_quarter, up_part, down_part = refs[count : count + 5]
    outs = refs[count + 5 : -1]
    stacked = refs[-1]
    old = (t - 1) * plan.rank
    if count == 1:
        stacked[:old, : plan.part] = pieces[0][...]
    else:
        for k, piece in enumerate(pieces):
            start = pl.multiple_of((quarter ^ k) * plan.width, LANES)
            stacked[:old, pl.ds(start, plan.width)] = piece[...]
    stacked[old:, : plan.part] = up_part[t - 1]

    def compute(held):
        rows = stacked[:, : plan.part]
        bend = nt(rows, down_part[t]).astype(BF16)
        value = nn(rows, held[...].reshape(plan.part, plan.wide)) + nn(bend, up_quarter[t])
        value = value.astype(BF16)
        if split:
            for m, out in enumerate(outs):
                out[...] = value[:, m * plan.width : (m + 1) * plan.width]
        else:
            outs[0][...] = value

    @pl.when(ic == t % plan.nc)
    def _():
        compute(mine)

    @pl.when(ic != t % plan.nc)
    def _():
        compute(twin)


def add_carried(plan, where, *refs):
    quarter, ic = where[0], where[4]
    ins, outs, rows = refs[: plan.nz], refs[plan.nz : -1], refs[-1]
    for j in range(plan.nz):
        total = 0.0
        for m in range(plan.nz):
            total = total + ins[m][:, (j ^ m) * plan.width : ((j ^ m) + 1) * plan.width].astype(F32)
        rows[:, j * plan.width : (j + 1) * plan.width] = total.astype(BF16)
    for k, out in enumerate(outs):
        target = jnp.minimum((quarter ^ k) // plan.nx * plan.nc + ic, plan.sections - 2)
        out[...] = rows[pl.ds(pl.multiple_of(target * plan.rank, plan.rank), plan.rank), :]


def top_rows(plan, where, *refs):
    grad, act, top_terms, squares = refs
    for m in range(plan.slots):
        where_rows = slice(m * plan.positions, (m + 1) * plan.positions)
        top = nn(act[:, where_rows], grad[where_rows, :])
        top_terms[m] = top
        squares[m : m + 1, :] = jnp.full((1, LANES), jnp.sum(top * top), F32)


def own_terms(plan, where, *refs):
    quarter, iz, section = where[0], where[1], where[2]
    pieces = refs[: plan.quarters]
    up_rows, grad, inputs, live, top_squares = refs[plan.quarters : plan.quarters + 5]
    down_terms, squares, carried = refs[plan.quarters + 5 :]
    last = section == plan.sections - 1
    for k, piece in enumerate(pieces):
        for m in range(plan.nz):
            for h in range(plan.width // LANES):
                low, there = plan.lane(quarter ^ k, h)
                start = pl.multiple_of((iz ^ m) * plan.part + low, LANES)

                @pl.when(there)
                def _():
                    at = m * plan.width + h * LANES
                    carried[:, pl.ds(start, LANES)] = piece[:, at : at + LANES]

    @pl.when(last)
    def _():
        carried[...] = up_rows[...]

    up_grad = (nt(carried[...], grad[...]).astype(BF16).astype(F32) * live[...]).astype(BF16)
    for m in range(plan.slots):
        where_rows = slice(m * plan.positions, (m + 1) * plan.positions)
        down = nn(up_grad[:, where_rows], inputs[where_rows, :])
        down_terms[m] = down
        total = jnp.full((1, LANES), jnp.sum(down * down), F32)
        squares[m : m + 1, :] = total + jnp.where(last, top_squares[m : m + 1, :], 0.0)


def on_device(acts, cotangent, frozen, down_adapter, up_adapter, example_ids, lengths):
    sizes = [lax.axis_size(name) for name in ("y", "c", "z", "x")]
    ny, nc, nz, nx = sizes
    iy, ic, iz, ix = (lax.axis_index(name) for name in ("y", "c", "z", "x"))
    inputs, weight = acts[0], frozen[0]
    down_rows, up_rows = down_adapter[0], up_adapter[0]
    slots = example_ids.shape[1]
    tokens, features = inputs.shape
    positions, rank, block = tokens // slots, down_rows.shape[0], weight.shape[0]
    plan = Plan(sizes, features, rank, slots, positions, block)
    sections, replicas, quarters = plan.sections, plan.replicas, plan.quarters
    part, width, wide, half = plan.part, plan.width, plan.wide, plan.half
    section = iy * nc + ic
    quarter = iy * nx + ix
    replica = iz * nx + ix
    where = jnp.stack([quarter, iz, section, iy, ic, ix, replica]).astype(jnp.int32)
    last = section == sections - 1

    def run(body, arrays, shapes, scratch=(), specs=None, extra=(), after=()):
        def kernel(at, *refs):
            body(plan, *extra, at, *refs[len(after) :])

        specs = [VMEM] * len(arrays) if specs is None else specs
        specs = [pl.BlockSpec(memory_space=pl.ANY)] * len(after) + specs
        arrays = list(after) + list(arrays)
        return local_call(kernel, where, arrays, shapes, scratch, specs)

    choose = (example_ids[0][:, None] == jnp.arange(slots, dtype=jnp.int32)[None, :]).astype(jnp.int32)
    slot_length = jnp.sum(choose * lengths[0][None, :], axis=1)
    live = jnp.arange(positions, dtype=jnp.int32)[None, :] < slot_length[:, None]
    live = live.astype(F32).reshape(1, tokens)
    clip_scale = math.sqrt(2.0 * rank * features) / math.sqrt(replicas * slots)

    down_act = (nt(down_rows, inputs).astype(BF16).astype(F32) * live).astype(BF16)
    own_up = lax.dynamic_slice_in_dim(up_rows, replica * block, block, 1)
    own_down = lax.dynamic_slice_in_dim(down_rows, replica * block, block, 1)
    act_known = jnp.concatenate([down_act, own_up], axis=1)
    act_all = [act_known] + [xor_permute(act_known, ("y", "c"), sections, j) for j in range(1, sections)]

    def cut(after):
        return run(cut_weight, [weight], [shape_of((block, wide))] * quarters, after=after)

    pieces = cut(act_all[1:])

    outs = run(
        first_rows,
        act_all + [cotangent, weight, up_rows, own_down],
        [
            shape_of((replicas, plan.group + rank, wide)),
            shape_of((replicas, (sections - 2) * plan.group, wide)),
        ],
        scratch=[
            pltpu.VMEM((sections, rank, tokens + block), BF16),
            pltpu.VMEM((nz, (sections - 1) * plan.group, part), BF16),
            pltpu.VMEM((rank, features), BF16),
        ],
        after=[pieces[1]],
    )
    lead = lax.all_to_all(outs[0], ("z", "x"), split_axis=0, concat_axis=0)

    def send_weight(pieces, core, step):
        pairs = []
        for y in range(ny):
            for x in range(nx):
                if y * nc + core > 0:
                    other = (y * nx + x) ^ step
                    pairs.append(
                        (((y * nc + core) * nx) + x, ((other // nx) * nc + core) * nx + other % nx)
                    )
        return lax.ppermute(pieces[step], ("y", "c", "x"), pairs)

    start = lax.dynamic_slice_in_dim(down_rows, iz * part, part, 1)
    adapters = jnp.concatenate([up_rows, start], axis=1)
    known = [adapters] + [xor_permute(adapters, ("y", "c"), sections, j) for j in range(1, sections)]
    up_quarter, up_part, down_part = run(
        sort_adapters,
        known,
        [shape_of((sections, rank, wide)), shape_of((sections, rank, part)), shape_of((sections, rank, part))],
        after=[outs[0]],
    )

    own, twin = {}, {}

    def share(core, pieces, after):
        held = [pieces[0]] + [send_weight(pieces, core, step) for step in range(1, quarters)]
        rows = [y for y in range(ny - 1, -1, -1) if y * nc + core > 0]
        found = run(collect, held, [shape_of((nx, block, wide))] * len(rows), extra=(rows,), after=after)
        for y, value in zip(rows, found):
            own[y * nc + core] = value
            twin[y * nc + core] = lax.ppermute(value, "c", [(core, c) for c in range(nc) if c != core])

    share(nc - 1, pieces, [up_quarter])

    finals = {}

    def stage(t, rows, after=()):
        count, height = len(rows), rows[0].shape[0]
        made = run(
            stage_rows,
            rows + [own[t], twin[t], up_quarter, down_part],
            [shape_of((height, width))] * quarters,
            scratch=[
                pltpu.VMEM((height if count > 1 else 8, wide), BF16),
                pltpu.VMEM((quarters, height, width), BF16),
            ],
            specs=[VMEM] * count + [VMEM, VMEM] + [VMEM, VMEM],
            extra=(t, count),
            after=after,
        )
        total = made[0].astype(F32)
        for step in range(1, quarters):
            total = total + xor_permute(made[step], ("y", "x"), quarters, step).astype(F32)
        return total, made[0]

    def to_parts(keep):
        mine = keep.astype(BF16)
        return [mine] + [xor_permute(mine, "z", nz, m) for m in range(1, nz)]

    top_terms, top_squares = run(
        top_rows, [cotangent, down_act], [shape_of((slots, rank, features), F32), shape_of((slots, LANES), F32)]
    )
    marks, sent = {}, {}
    rows = [lead[:, : plan.group].reshape(replicas * plan.group, wide)]
    for t in range(sections - 1, 0, -1):
        total, marks[t] = stage(t, rows)
        if t > 1:
            rows = to_parts(total)
            sent[t] = rows[0]
        if t == sections - 1:
            for core in range(nc - 2, -1, -1):
                share(core, pieces, [sent[t], top_squares])
    finals[0] = total
    rows = lax.all_to_all(outs[1], ("z", "x"), split_axis=0, concat_axis=0)
    rows = [rows.reshape(-1, wide)]
    for t in range(sections - 1, 1, -1):
        total, _ = stage(t, rows, [sent[t]])
        total = total.reshape(replicas, t - 1, plan.group, width)
        finals[t - 1] = total[:, -1]
        if t > 2:
            rows = to_parts(total[:, :-1].reshape(-1, width))

    seed = jnp.sum(lead[:, plan.group :].astype(F32), axis=0).astype(BF16)
    seed = lax.dynamic_slice_in_dim(seed, replica * block % LANES, block, 1)
    other = lax.ppermute(seed, "c", [(1 % nc, c) for c in range(nc) if c != 1 % nc])
    seed = jnp.where(ic == 1 % nc, seed, other)
    seeds = [seed] + [xor_permute(seed, ("y", "x"), quarters, k) for k in range(1, quarters)]
    seeds = jnp.stack(seeds)
    home = (1 // nc) * nx
    prefix = [
        jnp.concatenate(
            [lax.dynamic_index_in_dim(seeds, quarter ^ (home + x), 0, keepdims=False) for x in range(nx)], axis=1
        )
    ]
    for t in range(2, sections):
        split = t < sections - 1
        count = len(prefix)
        height = t * rank
        made = run(
            carry_rows,
            prefix + [own[t], twin[t], up_quarter, up_part, down_part],
            [shape_of((height, width))] * nz if split else [shape_of((height, wide))],
            scratch=[pltpu.VMEM((height, width * quarters), BF16)],
            specs=[VMEM] * count + [VMEM, VMEM] + [VMEM] * 3,
            extra=(t, count, split),
            after=[sent[sections + 1 - t]],
        )
        if split:
            total = made[0].astype(F32)
            for m in range(1, nz):
                total = total + xor_permute(made[m], "z", nz, m).astype(F32)
            total = total.astype(BF16)
            prefix = [total] + [xor_permute(total, ("y", "x"), quarters, k) for k in range(1, quarters)]
        else:
            others = [xor_permute(made[0], "z", nz, m) for m in range(1, nz)]
            picked = run(
                add_carried,
                [made[0]] + others,
                [shape_of((rank, wide))] * quarters,
                scratch=[pltpu.VMEM((height, wide), BF16)],
                after=[marks[1]],
            )
            prefix = [picked[0]] + [
                xor_permute(picked[k], ("y", "x"), quarters, k) for k in range(1, quarters)
            ]

    down_terms, own_squares = run(
        own_terms,
        prefix + [up_rows, cotangent, inputs, live, top_squares],
        [shape_of((slots, rank, features), F32), shape_of((slots, LANES), F32)],
        scratch=[pltpu.VMEM((rank, features), BF16)],
        after=[marks[1]],
    )

    mine = (jnp.arange(replicas) == replica).astype(F32)[:, None] * own_squares[:, 0][None, :]
    carried = {s: finals[s].reshape(replicas, half, rank, width) for s in finals}
    squares = sum(jnp.sum(value * value, axis=(2, 3)) for value in carried.values())
    squares = (jnp.arange(nc) == ic).astype(F32)[None, :, None] * squares[:, None, :]
    squares = (mine + squares.reshape(replicas, slots)).reshape(1, 1, replicas * slots)
    squares = jnp.broadcast_to(squares, (sections * replicas, 8, replicas * slots))
    squares = lax.all_to_all(squares, ("y", "c", "z", "x"), split_axis=0, concat_axis=0)
    totals = jnp.sum(squares[:, 0], axis=0).reshape(replicas, slots)
    norms = jnp.sqrt(totals)
    factors = clip_scale / (norms + 0.01)

    own_norms = lax.dynamic_index_in_dim(norms, replica, 0, keepdims=False)
    own_factors = lax.dynamic_index_in_dim(factors, replica, 0, keepdims=False)[:, None, None]
    sums = jnp.stack([jnp.sum(own_factors * down_terms, axis=0), jnp.sum(own_factors * top_terms, axis=0)])
    sums = sums.astype(BF16).reshape(2 * rank, replicas, block).transpose(1, 0, 2)
    sums = lax.all_to_all(sums, ("z", "x"), split_axis=0, concat_axis=0)
    sums = jnp.sum(sums.astype(F32), axis=0)
    grad_down, top_up = sums[:rank], sums[rank:]

    core_factors = lax.dynamic_index_in_dim(factors.reshape(replicas, nc, half), ic, 1, keepdims=False)
    scaled = [jnp.sum(core_factors[:, :, None, None] * carried[s], axis=(0, 1)) for s in range(sections - 1)]
    scaled.append(jnp.zeros_like(scaled[0]))
    scaled = jnp.stack(scaled)
    place = section * nx + ix
    found = []
    for k in range(sections * nx):
        part_rows = lax.dynamic_index_in_dim(scaled, (place ^ k) // nx, 0, keepdims=False)
        found.append(part_rows if k == 0 else xor_permute(part_rows, ("y", "c", "x"), sections * nx, k))
    found = jnp.stack(found).reshape(ny, nc, nx, rank, width)
    found = jnp.sum(found, axis=1).reshape(quarters, rank, width)
    scaled = jnp.concatenate(
        [lax.dynamic_index_in_dim(found, quarter ^ q, 0, keepdims=False) for q in range(quarters)], axis=1
    )
    low_up = lax.dynamic_slice_in_dim(scaled, ix * block, block, 1)
    grad_up = jnp.where(last, top_up, low_up)
    example_norms = jnp.sum(choose.astype(F32) * own_norms[:, None], axis=0)
    return (grad_down[None], grad_up[None], example_norms[None])


def solution(mesh):
    sections, replicas = mesh.shape["section"], mesh.shape["dp"]
    nc = 2
    ny = sections // nc
    nx = ny
    nz = replicas // nx
    fine = Mesh(mesh.devices.reshape(ny, nc, nz, nx), ("y", "c", "z", "x"))
    section, dp = ("y", "c"), ("z", "x")
    in_specs = (
        P(section, dp, None),
        P(dp, None),
        P(section, dp, None),
        P(section, None, None),
        P(section, None, None),
        P(dp, None),
        P(dp, None),
    )
    out_specs = (P(section, None, dp), P(section, None, dp), P(dp, None))

    return jax.shard_map(on_device, mesh=fine, in_specs=in_specs, out_specs=out_specs, check_vma=False)
```

```python
import math

import jax
import jax.numpy as jnp
from jax import lax
from jax.experimental import pallas as pl
from jax.experimental.pallas import tpu as pltpu
from jax.sharding import Mesh, PartitionSpec as P

LANES = 128
BF16 = jnp.bfloat16
F32 = jnp.float32
VMEM = pl.BlockSpec(memory_space=pltpu.VMEM)
SMEM = pl.BlockSpec(memory_space=pltpu.SMEM)


def mm(left, right, dims):
    return lax.dot_general(left, right, (dims, ((), ())), preferred_element_type=F32)


def nt(left, right):
    return mm(left, right, ((1,), (1,)))


def nn(left, right):
    return mm(left, right, ((1,), (0,)))


def local_call(body, where, arrays, shapes, scratch=(), specs=None):
    specs = [VMEM] * len(arrays) if specs is None else specs
    return pl.pallas_call(
        body,
        out_shape=shapes,
        grid=(1,),
        in_specs=[SMEM] + specs,
        out_specs=[VMEM] * len(shapes),
        scratch_shapes=list(scratch),
        compiler_params=pltpu.CompilerParams(vmem_limit_bytes=56 * 1024 * 1024),
    )(where, *arrays)


def shape_of(dims, dtype=BF16):
    return jax.ShapeDtypeStruct(dims, dtype)


def xor_permute(value, axes, count, step):
    return lax.ppermute(value, axes, [(i, i ^ step) for i in range(count)])


class Plan:
    def __init__(self, sizes, features, rank, slots, positions, block):
        self.ny, self.nc, self.nz, self.nx = sizes
        self.sections, self.replicas = self.ny * self.nc, self.nz * self.nx
        self.quarters = self.ny * self.nx
        self.features, self.rank, self.slots, self.positions = features, rank, slots, positions
        self.block = block
        self.part = features // self.nz
        self.width = -(-self.part // (self.quarters * LANES)) * LANES
        self.wide = self.nz * self.width
        self.half = slots // self.nc
        self.group = self.half * rank
        self.height = self.group * self.replicas

    def window(self, replica):
        low = replica * self.block // LANES * LANES
        return low, min(-(-self.block // LANES) * LANES, self.features - low)

    def lane(self, quarter, step):
        low = quarter * self.width + step * LANES
        return jnp.minimum(low, self.part - LANES), low < self.part


def cut_weight(plan, where, weight_ref, *outs):
    quarter, iz = where[0], where[1]
    for k, out in enumerate(outs):
        for m in range(plan.nz):
            for h in range(plan.width // LANES):
                low, _ = plan.lane(quarter ^ k, h)
                start = pl.multiple_of((iz ^ m) * plan.part + low, LANES)
                lanes = slice(m * plan.width + h * LANES, m * plan.width + (h + 1) * LANES)
                out[:, lanes] = weight_ref[:, pl.ds(start, LANES)]


def sort_adapters(plan, where, *refs):
    quarter, iz, section = where[0], where[1], where[2]
    ins, (up_quarter, up_part, down_part) = refs[: plan.sections], refs[plan.sections :]
    for j, known in enumerate(ins):
        s = section ^ j
        for m in range(plan.nz):
            for h in range(plan.width // LANES):
                low, _ = plan.lane(quarter, h)
                start = pl.multiple_of((iz ^ m) * plan.part + low, LANES)
                lanes = slice(m * plan.width + h * LANES, m * plan.width + (h + 1) * LANES)
                up_quarter[s, :, lanes] = known[:, pl.ds(start, LANES)]
        start = pl.multiple_of(iz * plan.part, LANES)
        up_part[s] = known[:, pl.ds(start, plan.part)]
        down_part[s] = known[:, plan.features :]


def collect(plan, stages, where, *refs):
    pieces, outs = refs[: plan.quarters], refs[plan.quarters :]
    for k, piece in enumerate(pieces):
        source = where[0] ^ k
        for y, out in zip(stages, outs):

            @pl.when(source // plan.nx == y)
            def _():
                out[source % plan.nx] = piece[...]


def first_rows(plan, where, *refs):
    iz, section, iy, ic, ix, replica = where[1], where[2], where[3], where[4], where[5], where[6]
    tokens = plan.slots * plan.positions
    known_acts = refs[: plan.sections]
    grad, weight, up_rows, own_down, live, low_out, high_out, act, rows, seeds = refs[plan.sections :]
    for j, known in enumerate(known_acts):
        act[section ^ j] = known[...]
    for i in range(plan.half):
        start = pl.multiple_of((ic * plan.half + i) * plan.positions, plan.positions)
        left = jnp.concatenate([act[s, :, pl.ds(start, plan.positions)] for s in range(plan.sections - 1)], axis=0)
        left = (left.astype(F32) * live[:, pl.ds(start, plan.positions)]).astype(BF16)
        for m in range(plan.nz):
            lanes = pl.multiple_of((iz ^ m) * plan.part, LANES)
            right = grad[pl.ds(start, plan.positions), pl.ds(lanes, plan.part)]
            made = nn(left, right).astype(BF16)
            for s in range(plan.sections - 1):
                low = s * plan.group + i * plan.rank
                rows[m, low : low + plan.rank, :] = made[s * plan.rank : (s + 1) * plan.rank]
    start_rows = act[0, :, tokens : tokens + plan.block]
    seed = nn(start_rows, weight[...]) + nn(nt(start_rows, own_down[...]).astype(BF16), up_rows[...])
    seeds[...] = seed.astype(BF16)
    for d in range(plan.replicas):
        low, window = plan.window(d)
        low_out[d, plan.group :, :window] = seeds[:, low : low + window]
    for kx in range(plan.nx):
        quarter = iy * plan.nx + (ix ^ kx)
        for m in range(plan.nz):
            for h in range(plan.width // LANES):
                low, there = plan.lane(quarter, h)
                tile = rows[m, :, pl.ds(pl.multiple_of(low, LANES), LANES)]
                tile = jnp.where(there, tile, jnp.zeros_like(tile))
                for kz in range(plan.nz):
                    at = (kz ^ m) * plan.width + h * LANES
                    there_index = replica ^ (kz * plan.nx + kx)
                    low_out[there_index, : plan.group, at : at + LANES] = tile[: plan.group]
                    high_out[there_index, :, at : at + LANES] = tile[plan.group :]


def stage_rows(plan, t, count, where, *refs):
    quarter, ic = where[0], where[4]
    pieces = refs[:count]
    mine, twin, up_quarter, down_part = refs[count : count + 4]
    outs = refs[count + 4 : count + 4 + plan.quarters]
    flat, made = refs[count + 4 + plan.quarters :]
    if count == 1:
        flat = pieces[0]
    else:
        for j, piece in enumerate(pieces):
            flat[:, j * plan.width : (j + 1) * plan.width] = piece[...]
    tall = plan.height

    def compute(held):
        def tile(index, carry):
            at = pl.ds(pl.multiple_of(index * tall, tall), tall)
            rows = flat[at, :]
            bend = nt(rows, up_quarter[t]).astype(BF16)
            matrix = held[...].reshape(plan.part, plan.wide)
            for q in range(plan.quarters):
                low, high = min(q * plan.width, plan.part), min((q + 1) * plan.width, plan.part)
                if high > low:
                    value = nt(rows, matrix[low:high]) + nn(bend, down_part[t, :, low:high])
                    made[quarter ^ q, at, : high - low] = value.astype(BF16)
                if high - low < plan.width:
                    made[quarter ^ q, at, high - low :] = jnp.zeros((tall, plan.width - (high - low)), BF16)
            return carry

        lax.fori_loop(0, flat.shape[0] // tall, tile, 0)

    @pl.when(ic == t % plan.nc)
    def _():
        compute(mine)

    @pl.when(ic != t % plan.nc)
    def _():
        compute(twin)

    for k, out in enumerate(outs):
        out[...] = made[k]


def carry_rows(plan, t, count, split, where, *refs):
    quarter, ic = where[0], where[4]
    pieces = refs[:count]
    mine, twin, up_quarter, up_part, down_part = refs[count : count + 5]
    outs = refs[count + 5 : -1]
    stacked = refs[-1]
    old = (t - 1) * plan.rank
    if count == 1:
        stacked[:old, : plan.part] = pieces[0][...]
    else:
        for k, piece in enumerate(pieces):
            start = pl.multiple_of((quarter ^ k) * plan.width, LANES)
            stacked[:old, pl.ds(start, plan.width)] = piece[...]
    stacked[old:, : plan.part] = up_part[t - 1]

    def compute(held):
        rows = stacked[:, : plan.part]
        bend = nt(rows, down_part[t]).astype(BF16)
        value = nn(rows, held[...].reshape(plan.part, plan.wide)) + nn(bend, up_quarter[t])
        value = value.astype(BF16)
        if split:
            for m, out in enumerate(outs):
                out[...] = value[:, m * plan.width : (m + 1) * plan.width]
        else:
            outs[0][...] = value

    @pl.when(ic == t % plan.nc)
    def _():
        compute(mine)

    @pl.when(ic != t % plan.nc)
    def _():
        compute(twin)


def add_carried(plan, where, *refs):
    quarter, ic = where[0], where[4]
    ins, outs, rows = refs[: plan.nz], refs[plan.nz : -1], refs[-1]
    for j in range(plan.nz):
        total = 0.0
        for m in range(plan.nz):
            total = total + ins[m][:, (j ^ m) * plan.width : ((j ^ m) + 1) * plan.width].astype(F32)
        rows[:, j * plan.width : (j + 1) * plan.width] = total.astype(BF16)
    for k, out in enumerate(outs):
        target = jnp.minimum((quarter ^ k) // plan.nx * plan.nc + ic, plan.sections - 2)
        out[...] = rows[pl.ds(pl.multiple_of(target * plan.rank, plan.rank), plan.rank), :]


def top_rows(plan, where, *refs):
    grad, act, top_terms, squares = refs
    for m in range(plan.slots):
        where_rows = slice(m * plan.positions, (m + 1) * plan.positions)
        top = nn(act[:, where_rows], grad[where_rows, :])
        top_terms[m] = top
        squares[m : m + 1, :] = jnp.full((1, LANES), jnp.sum(top * top), F32)


def own_terms(plan, where, *refs):
    quarter, iz, section = where[0], where[1], where[2]
    pieces = refs[: plan.quarters]
    up_rows, grad, inputs, live, top_squares = refs[plan.quarters : plan.quarters + 5]
    down_terms, squares, carried = refs[plan.quarters + 5 :]
    last = section == plan.sections - 1
    for k, piece in enumerate(pieces):
        for m in range(plan.nz):
            for h in range(plan.width // LANES):
                low, there = plan.lane(quarter ^ k, h)
                start = pl.multiple_of((iz ^ m) * plan.part + low, LANES)

                @pl.when(there)
                def _():
                    at = m * plan.width + h * LANES
                    carried[:, pl.ds(start, LANES)] = piece[:, at : at + LANES]

    @pl.when(last)
    def _():
        carried[...] = up_rows[...]

    up_grad = (nt(carried[...], grad[...]).astype(BF16).astype(F32) * live[...]).astype(BF16)
    for m in range(plan.slots):
        where_rows = slice(m * plan.positions, (m + 1) * plan.positions)
        down = nn(up_grad[:, where_rows], inputs[where_rows, :])
        down_terms[m] = down
        total = jnp.full((1, LANES), jnp.sum(down * down), F32)
        squares[m : m + 1, :] = total + jnp.where(last, top_squares[m : m + 1, :], 0.0)


def on_device(acts, cotangent, frozen, down_adapter, up_adapter, example_ids, lengths):
    sizes = [lax.axis_size(name) for name in ("y", "c", "z", "x")]
    ny, nc, nz, nx = sizes
    iy, ic, iz, ix = (lax.axis_index(name) for name in ("y", "c", "z", "x"))
    inputs, weight = acts[0], frozen[0]
    down_rows, up_rows = down_adapter[0], up_adapter[0]
    slots = example_ids.shape[1]
    tokens, features = inputs.shape
    positions, rank, block = tokens // slots, down_rows.shape[0], weight.shape[0]
    plan = Plan(sizes, features, rank, slots, positions, block)
    sections, replicas, quarters = plan.sections, plan.replicas, plan.quarters
    part, width, wide, half = plan.part, plan.width, plan.wide, plan.half
    section = iy * nc + ic
    quarter = iy * nx + ix
    replica = iz * nx + ix
    where = jnp.stack([quarter, iz, section, iy, ic, ix, replica]).astype(jnp.int32)
    last = section == sections - 1

    def run(body, arrays, shapes, scratch=(), specs=None, extra=(), after=()):
        def kernel(at, *refs):
            body(plan, *extra, at, *refs[len(after) :])

        specs = [VMEM] * len(arrays) if specs is None else specs
        specs = [pl.BlockSpec(memory_space=pl.ANY)] * len(after) + specs
        arrays = list(after) + list(arrays)
        return local_call(kernel, where, arrays, shapes, scratch, specs)

    choose = (example_ids[0][:, None] == jnp.arange(slots, dtype=jnp.int32)[None, :]).astype(jnp.int32)
    slot_length = jnp.sum(choose * lengths[0][None, :], axis=1)
    live = jnp.arange(positions, dtype=jnp.int32)[None, :] < slot_length[:, None]
    live = live.astype(F32).reshape(1, tokens)
    clip_scale = math.sqrt(2.0 * rank * features) / math.sqrt(replicas * slots)

    all_act = nt(down_rows, inputs).astype(BF16)
    down_act = (all_act.astype(F32) * live).astype(BF16)
    own_up = lax.dynamic_slice_in_dim(up_rows, replica * block, block, 1)
    own_down = lax.dynamic_slice_in_dim(down_rows, replica * block, block, 1)
    act_known = jnp.concatenate([all_act, own_up], axis=1)
    act_all = [act_known] + [xor_permute(act_known, ("y", "c"), sections, j) for j in range(1, sections)]

    def cut(after):
        return run(cut_weight, [weight], [shape_of((block, wide))] * quarters, after=after)

    pieces = cut(act_all[1:])

    outs = run(
        first_rows,
        act_all + [cotangent, weight, up_rows, own_down, live],
        [
            shape_of((replicas, plan.group + rank, wide)),
            shape_of((replicas, (sections - 2) * plan.group, wide)),
        ],
        scratch=[
            pltpu.VMEM((sections, rank, tokens + block), BF16),
            pltpu.VMEM((nz, (sections - 1) * plan.group, part), BF16),
            pltpu.VMEM((rank, features), BF16),
        ],
        after=[pieces[1]],
    )
    lead = lax.all_to_all(outs[0], ("z", "x"), split_axis=0, concat_axis=0)

    def send_weight(pieces, core, step):
        pairs = []
        for y in range(ny):
            for x in range(nx):
                if y * nc + core > 0:
                    other = (y * nx + x) ^ step
                    pairs.append(
                        (((y * nc + core) * nx) + x, ((other // nx) * nc + core) * nx + other % nx)
                    )
        return lax.ppermute(pieces[step], ("y", "c", "x"), pairs)

    start = lax.dynamic_slice_in_dim(down_rows, iz * part, part, 1)
    adapters = jnp.concatenate([up_rows, start], axis=1)
    known = [adapters] + [xor_permute(adapters, ("y", "c"), sections, j) for j in range(1, sections)]
    up_quarter, up_part, down_part = run(
        sort_adapters,
        known,
        [shape_of((sections, rank, wide)), shape_of((sections, rank, part)), shape_of((sections, rank, part))],
        after=[outs[0]],
    )

    own, twin = {}, {}

    def share(core, pieces, after):
        held = [pieces[0]] + [send_weight(pieces, core, step) for step in range(1, quarters)]
        rows = [y for y in range(ny - 1, -1, -1) if y * nc + core > 0]
        found = run(collect, held, [shape_of((nx, block, wide))] * len(rows), extra=(rows,), after=after)
        for y, value in zip(rows, found):
            own[y * nc + core] = value
            twin[y * nc + core] = lax.ppermute(value, "c", [(core, c) for c in range(nc) if c != core])

    share(nc - 1, pieces, [up_quarter])

    finals = {}

    def stage(t, rows, after=()):
        count, height = len(rows), rows[0].shape[0]
        made = run(
            stage_rows,
            rows + [own[t], twin[t], up_quarter, down_part],
            [shape_of((height, width))] * quarters,
            scratch=[
                pltpu.VMEM((height if count > 1 else 8, wide), BF16),
                pltpu.VMEM((quarters, height, width), BF16),
            ],
            specs=[VMEM] * count + [VMEM, VMEM] + [VMEM, VMEM],
            extra=(t, count),
            after=after,
        )
        total = made[0].astype(F32)
        for step in range(1, quarters):
            total = total + xor_permute(made[step], ("y", "x"), quarters, step).astype(F32)
        return total, made[0]

    def to_parts(keep):
        mine = keep.astype(BF16)
        return [mine] + [xor_permute(mine, "z", nz, m) for m in range(1, nz)]

    top_terms, top_squares = run(
        top_rows, [cotangent, down_act], [shape_of((slots, rank, features), F32), shape_of((slots, LANES), F32)]
    )
    marks, sent = {}, {}
    rows = [lead[:, : plan.group].reshape(replicas * plan.group, wide)]
    for t in range(sections - 1, 0, -1):
        total, marks[t] = stage(t, rows)
        if t > 1:
            rows = to_parts(total)
            sent[t] = rows[0]
        if t == sections - 1:
            for core in range(nc - 2, -1, -1):
                share(core, pieces, [sent[t], top_squares])
    finals[0] = total
    rows = lax.all_to_all(outs[1], ("z", "x"), split_axis=0, concat_axis=0)
    rows = [rows.reshape(-1, wide)]
    for t in range(sections - 1, 1, -1):
        total, _ = stage(t, rows, [sent[t]])
        total = total.reshape(replicas, t - 1, plan.group, width)
        finals[t - 1] = total[:, -1]
        if t > 2:
            rows = to_parts(total[:, :-1].reshape(-1, width))

    seed = jnp.sum(lead[:, plan.group :].astype(F32), axis=0).astype(BF16)
    seed = lax.dynamic_slice_in_dim(seed, replica * block % LANES, block, 1)
    other = lax.ppermute(seed, "c", [(1 % nc, c) for c in range(nc) if c != 1 % nc])
    seed = jnp.where(ic == 1 % nc, seed, other)
    seeds = [seed] + [xor_permute(seed, ("y", "x"), quarters, k) for k in range(1, quarters)]
    seeds = jnp.stack(seeds)
    home = (1 // nc) * nx
    prefix = [
        jnp.concatenate(
            [lax.dynamic_index_in_dim(seeds, quarter ^ (home + x), 0, keepdims=False) for x in range(nx)], axis=1
        )
    ]
    for t in range(2, sections):
        split = t < sections - 1
        count = len(prefix)
        height = t * rank
        made = run(
            carry_rows,
            prefix + [own[t], twin[t], up_quarter, up_part, down_part],
            [shape_of((height, width))] * nz if split else [shape_of((height, wide))],
            scratch=[pltpu.VMEM((height, width * quarters), BF16)],
            specs=[VMEM] * count + [VMEM, VMEM] + [VMEM] * 3,
            extra=(t, count, split),
            after=[sent[sections + 1 - t]],
        )
        if split:
            total = made[0].astype(F32)
            for m in range(1, nz):
                total = total + xor_permute(made[m], "z", nz, m).astype(F32)
            total = total.astype(BF16)
            prefix = [total] + [xor_permute(total, ("y", "x"), quarters, k) for k in range(1, quarters)]
        else:
            others = [xor_permute(made[0], "z", nz, m) for m in range(1, nz)]
            picked = run(
                add_carried,
                [made[0]] + others,
                [shape_of((rank, wide))] * quarters,
                scratch=[pltpu.VMEM((height, wide), BF16)],
                after=[marks[1]],
            )
            prefix = [picked[0]] + [
                xor_permute(picked[k], ("y", "x"), quarters, k) for k in range(1, quarters)
            ]

    down_terms, own_squares = run(
        own_terms,
        prefix + [up_rows, cotangent, inputs, live, top_squares],
        [shape_of((slots, rank, features), F32), shape_of((slots, LANES), F32)],
        scratch=[pltpu.VMEM((rank, features), BF16)],
        after=[marks[1]],
    )

    mine = (jnp.arange(replicas) == replica).astype(F32)[:, None] * own_squares[:, 0][None, :]
    carried = {s: finals[s].reshape(replicas, half, rank, width) for s in finals}
    squares = sum(jnp.sum(value * value, axis=(2, 3)) for value in carried.values())
    squares = (jnp.arange(nc) == ic).astype(F32)[None, :, None] * squares[:, None, :]
    squares = (mine + squares.reshape(replicas, slots)).reshape(1, 1, replicas * slots)
    squares = jnp.broadcast_to(squares, (sections * replicas, 8, replicas * slots))
    squares = lax.all_to_all(squares, ("y", "c", "z", "x"), split_axis=0, concat_axis=0)
    totals = jnp.sum(squares[:, 0], axis=0).reshape(replicas, slots)
    norms = jnp.sqrt(totals)
    factors = clip_scale / (norms + 0.01)

    own_norms = lax.dynamic_index_in_dim(norms, replica, 0, keepdims=False)
    own_factors = lax.dynamic_index_in_dim(factors, replica, 0, keepdims=False)[:, None, None]
    sums = jnp.stack([jnp.sum(own_factors * down_terms, axis=0), jnp.sum(own_factors * top_terms, axis=0)])
    sums = sums.astype(BF16).reshape(2 * rank, replicas, block).transpose(1, 0, 2)
    sums = lax.all_to_all(sums, ("z", "x"), split_axis=0, concat_axis=0)
    sums = jnp.sum(sums.astype(F32), axis=0)
    grad_down, top_up = sums[:rank], sums[rank:]

    core_factors = lax.dynamic_index_in_dim(factors.reshape(replicas, nc, half), ic, 1, keepdims=False)
    scaled = [jnp.sum(core_factors[:, :, None, None] * carried[s], axis=(0, 1)) for s in range(sections - 1)]
    scaled.append(jnp.zeros_like(scaled[0]))
    scaled = jnp.stack(scaled)
    place = section * nx + ix
    found = []
    for k in range(sections * nx):
        part_rows = lax.dynamic_index_in_dim(scaled, (place ^ k) // nx, 0, keepdims=False)
        found.append(part_rows if k == 0 else xor_permute(part_rows, ("y", "c", "x"), sections * nx, k))
    found = jnp.stack(found).reshape(ny, nc, nx, rank, width)
    found = jnp.sum(found, axis=1).reshape(quarters, rank, width)
    scaled = jnp.concatenate(
        [lax.dynamic_index_in_dim(found, quarter ^ q, 0, keepdims=False) for q in range(quarters)], axis=1
    )
    low_up = lax.dynamic_slice_in_dim(scaled, ix * block, block, 1)
    grad_up = jnp.where(last, top_up, low_up)
    example_norms = jnp.sum(choose.astype(F32) * own_norms[:, None], axis=0)
    return (grad_down[None], grad_up[None], example_norms[None])


def solution(mesh):
    sections, replicas = mesh.shape["section"], mesh.shape["dp"]
    nc = 2
    ny = sections // nc
    nx = ny
    nz = replicas // nx
    fine = Mesh(mesh.devices.reshape(ny, nc, nz, nx), ("y", "c", "z", "x"))
    section, dp = ("y", "c"), ("z", "x")
    in_specs = (
        P(section, dp, None),
        P(dp, None),
        P(section, dp, None),
        P(section, None, None),
        P(section, None, None),
        P(dp, None),
        P(dp, None),
    )
    out_specs = (P(section, None, dp), P(section, None, dp), P(dp, None))

    return jax.shard_map(on_device, mesh=fine, in_specs=in_specs, out_specs=out_specs, check_vma=False)
```
